32 devices in a mesh: dp: 1 (over z), sp: 4 (over y), tp: 8 (over x, core).
Axes of the slice: x: 4, y: 4, z: 1, core: 2. Of those that a mesh axis runs over, the one named last changes fastest.
The devices are a block of a 4x4x8 slice.
Arguments:
- x_in: bfloat16 [128, 4096], P('dp')
- lengths: int32 [128], P('dp')
- w_q: bfloat16 [2, 4096, 4096], P(None, None, 'tp')
- w_k: bfloat16 [2, 4096, 1024], P(None, None, 'tp')
- w_v: bfloat16 [2, 4096, 1024], P(None, None, 'tp')
- w_o: bfloat16 [2, 4096, 4096], P(None, 'tp')
- w_gate: bfloat16 [2, 4096, 14336], P(None, None, 'tp')
- w_up: bfloat16 [2, 4096, 14336], P(None, None, 'tp')
- w_down: bfloat16 [2, 14336, 4096], P(None, 'tp')
- gain_attn: bfloat16 [2, 4096], replicated
- gain_mlp: bfloat16 [2, 4096], replicated
- k_cache: bfloat16 [2, 128, 8, 256, 128], P(None, 'dp', 'tp', 'sp')
- v_cache: bfloat16 [2, 128, 8, 256, 128], P(None, 'dp', 'tp', 'sp')
Outputs:
- output 1: bfloat16 [128, 4096], P('dp')
- output 2: bfloat16 [2, 128, 8, 128], P(None, 'dp', 'tp')
- output 3: bfloat16 [2, 128, 8, 128], P(None, 'dp', 'tp')
All inputs are finite; a program needn't handle non-finite values.
Results may differ from the reference program's by a relative error of at most 0.02.
Values are sent between devices in bfloat16 or wider.
A program may use at most 768 MiB of HBM per device.

```python
import math
import jax
import jax.numpy as jnp
from jax import lax

D = 4096
HQ = 32
HKV = 8
DH = 128
FF = 14336
LAYERS = 2
BATCH = 128
T_CACHE = 256

GROUP_SIZE = HQ // HKV
LOG_SPAN = int(math.log2(T_CACHE))
EPSILON = 1e-5
NEG_BIG = -1e30


def draw_lengths(len_key):
    key_uni, key_shift, key_base = jax.random.split(len_key, 3)
    uniform_len = jax.random.randint(key_uni, (BATCH,), 1, T_CACHE + 1)
    shift_amt = jax.random.randint(key_shift, (BATCH,), 0, LOG_SPAN + 1)
    short_len = 1 + jnp.right_shift(jax.random.randint(key_base, (BATCH,), 0, T_CACHE), shift_amt)
    seq_idx = jnp.arange(BATCH)
    seq_lens = jnp.where(seq_idx % 4 == 0, T_CACHE, jnp.where(seq_idx % 4 == 1, short_len, uniform_len))
    seq_lens = jnp.where(seq_idx == 1, 1, seq_lens)
    return seq_lens.astype(jnp.int32)


def normal_bf16(rand_key, arr_shape, weight_scale):
    return (jax.random.normal(rand_key, arr_shape, jnp.float32) * weight_scale).astype(jnp.bfloat16)


def setup_inputs(seed: int = 0, part: int = 0) -> dict:
    shared_keys = jax.random.split(jax.random.key(seed), 9)
    part_keys = jax.random.split(jax.random.fold_in(jax.random.key(seed + 1), part), 3)
    len_key = jax.random.fold_in(jax.random.key(seed + 2), part)
    gain_attn = (1.0 + 0.5 * jax.random.normal(shared_keys[7], (LAYERS, D), jnp.float32)).astype(jnp.bfloat16)
    gain_mlp = (1.0 + 0.5 * jax.random.normal(shared_keys[8], (LAYERS, D), jnp.float32)).astype(jnp.bfloat16)
    return {
        "x_in": normal_bf16(part_keys[0], (BATCH, D), 1.0),
        "lengths": draw_lengths(len_key),
        "w_q": normal_bf16(shared_keys[0], (LAYERS, D, HQ * DH), 3.0 * D ** -0.5),
        "w_k": normal_bf16(shared_keys[1], (LAYERS, D, HKV * DH), D ** -0.5),
        "w_v": normal_bf16(shared_keys[2], (LAYERS, D, HKV * DH), D ** -0.5),
        "w_o": normal_bf16(shared_keys[3], (LAYERS, HQ * DH, D), (HQ * DH) ** -0.5),
        "w_gate": normal_bf16(shared_keys[4], (LAYERS, D, FF), D ** -0.5),
        "w_up": normal_bf16(shared_keys[5], (LAYERS, D, FF), D ** -0.5),
        "w_down": normal_bf16(shared_keys[6], (LAYERS, FF, D), 1.5 * FF ** -0.5),
        "gain_attn": gain_attn,
        "gain_mlp": gain_mlp,
        "k_cache": normal_bf16(part_keys[1], (LAYERS, BATCH, HKV, T_CACHE, DH), 1.0),
        "v_cache": normal_bf16(part_keys[2], (LAYERS, BATCH, HKV, T_CACHE, DH), 1.0),
    }


def rms_norm(residual, gain_vec):
    wide_res = residual.astype(jnp.float32)
    mean_sq = jnp.mean(wide_res * wide_res, axis=-1, keepdims=True)
    return (wide_res * lax.rsqrt(mean_sq + EPSILON) * gain_vec.astype(jnp.float32)).astype(jnp.bfloat16)


def reference(x_in, lengths, w_q, w_k, w_v, w_o, w_gate, w_up, w_down, gain_attn, gain_mlp, k_cache, v_cache):
    positions = jnp.arange(T_CACHE)
    score_scale = DH ** -0.5

    def one_sequence(seq_args):
        q_row, k_row, v_row, k_seq, v_seq, seq_len = seq_args
        q_heads = q_row.reshape(HKV, GROUP_SIZE, DH).astype(jnp.float32)
        k_head = k_row.reshape(HKV, DH).astype(jnp.float32)
        v_head = v_row.reshape(HKV, DH).astype(jnp.float32)
        valid_mask = positions < seq_len
        scores = jnp.einsum("kgd,ktd->kgt", q_heads, k_seq.astype(jnp.float32)) * score_scale
        scores = jnp.where(valid_mask, scores, NEG_BIG)
        new_score = jnp.einsum("kgd,kd->kg", q_heads, k_head) * score_scale
        run_max = jnp.maximum(jnp.max(scores, axis=-1), new_score)
        prob_w = jnp.where(valid_mask, jnp.exp(scores - run_max[..., None]), 0.0)
        prob_new = jnp.exp(new_score - run_max)
        denom_sum = jnp.sum(prob_w, axis=-1) + prob_new
        numer_sum = jnp.einsum("kgt,ktd->kgd", prob_w.astype(jnp.bfloat16).astype(jnp.float32), v_seq.astype(jnp.float32))
        numer_sum = numer_sum + prob_new.astype(jnp.bfloat16).astype(jnp.float32)[..., None] * v_head[:, None, :]
        return (numer_sum / denom_sum[..., None]).astype(jnp.bfloat16).reshape(HQ * DH)

    def layer_step(residual, layer_args):
        q_weight, k_weight, v_weight, o_weight, gate_weight, up_weight, down_weight, attn_gain, mlp_gain, k_layer, v_layer = layer_args
        normed = rms_norm(residual, attn_gain)
        query_vec = jnp.dot(normed, q_weight, preferred_element_type=jnp.float32).astype(jnp.bfloat16)
        key_new = jnp.dot(normed, k_weight, preferred_element_type=jnp.float32).astype(jnp.bfloat16)
        val_new = jnp.dot(normed, v_weight, preferred_element_type=jnp.float32).astype(jnp.bfloat16)
        attn_out = lax.map(one_sequence, (query_vec, key_new, val_new, k_layer, v_layer, lengths))
        attn_sum = jnp.dot(attn_out, o_weight, preferred_element_type=jnp.float32)
        residual = (residual.astype(jnp.float32) + attn_sum).astype(jnp.bfloat16)
        normed_mlp = rms_norm(residual, mlp_gain)
        gate_proj = jnp.dot(normed_mlp, gate_weight, preferred_element_type=jnp.float32)
        up_proj = jnp.dot(normed_mlp, up_weight, preferred_element_type=jnp.float32)
        hidden_act = (jax.nn.silu(gate_proj) * up_proj).astype(jnp.bfloat16)
        mlp_sum = jnp.dot(hidden_act, down_weight, preferred_element_type=jnp.float32)
        residual = (residual.astype(jnp.float32) + mlp_sum).astype(jnp.bfloat16)
        return residual, (key_new.reshape(BATCH, HKV, DH), val_new.reshape(BATCH, HKV, DH))

    x_out, new_kv = lax.scan(layer_step, x_in, (w_q, w_k, w_v, w_o, w_gate, w_up, w_down, gain_attn, gain_mlp, k_cache, v_cache))
    return x_out, new_kv[0], new_kv[1]
```

```python
import functools

import jax
import jax.numpy as jnp
from jax import lax
from jax.experimental import pallas as pl
from jax.experimental.pallas import tpu as pltpu
from jax.sharding import PartitionSpec as P

EPSILON = 1e-5
NEG_BIG = -1e30
F32 = jnp.float32
BF16 = jnp.bfloat16
MESH = pl.DeviceIdType.MESH
VMEM_LIMIT = 67043328


def decode_kernel(
    n_sp, n_tp,
    len_ref, xin_hbm, wq_hbm, wk_hbm, wv_hbm, wo_hbm, wg_hbm, wu_hbm, wd_hbm, ga_ref, gm_ref, kc_hbm, vc_hbm,
    xo_ref, kn_ref, vn_ref,
    wqkv, wo, wg, wu, wd, kbuf, vbuf, xin, hrow, qkvf, qacc, snew, sbuf, obuf, stsend, orecv, strecv, o2d,
    gacc, uacc, act, psend, prev, precv, xres, xbuf,
    sem_x, sem_qkv, sem_wo, sem_wg, sem_wu, sem_wd, sem_kv,
    ys_send, ys_recv, yt_send, yt_recv, yq_send, yq_recv,
    rs_send, rs_recv, ag_send, ag_recv,
    f1_send, f1_recv, f2_send, f2_recv, f3_send, f3_recv,
):
    n_layers = wq_hbm.shape[0]
    batch, width = xin.shape
    head = kbuf.shape[1]
    qw = wq_hbm.shape[2]
    group = qw // head
    t_local = kbuf.shape[0] // batch
    rows = batch // n_sp
    cols = width // n_tp
    n_k = sem_qkv.shape[0]
    k_chunk = width // n_k
    n_gk = wg.shape[0]
    g_chunk = wg.shape[1]
    scale = head ** -0.5
    blk = rows * group
    sub = 16
    span = 4 * t_local
    s_idx = lax.axis_index("sp")
    i_idx = lax.axis_index("tp")

    def qkv_copies(l, c):
        ks = pl.ds(c * k_chunk, k_chunk)
        return (
            pltpu.make_async_copy(wq_hbm.at[l, ks, :], wqkv.at[ks, pl.ds(0, qw)], sem_qkv.at[c, 0]),
            pltpu.make_async_copy(wk_hbm.at[l, ks, :], wqkv.at[ks, pl.ds(qw, head)], sem_qkv.at[c, 1]),
            pltpu.make_async_copy(wv_hbm.at[l, ks, :], wqkv.at[ks, pl.ds(qw + head, head)], sem_qkv.at[c, 2]),
        )

    def wo_copy(l):
        return pltpu.make_async_copy(wo_hbm.at[l], wo, sem_wo)

    def wg_copy(l, c):
        return pltpu.make_async_copy(wg_hbm.at[l, pl.ds(c * g_chunk, g_chunk), :], wg.at[c], sem_wg.at[c])

    def wu_copy(l, c):
        return pltpu.make_async_copy(wu_hbm.at[l, pl.ds(c * g_chunk, g_chunk), :], wu.at[c], sem_wu.at[c])

    def wd_copy(l):
        return pltpu.make_async_copy(wd_hbm.at[l], wd, sem_wd)

    def kv_copies(l):
        return (
            pltpu.make_async_copy(kc_hbm.at[l], kbuf, sem_kv.at[0]),
            pltpu.make_async_copy(vc_hbm.at[l], vbuf, sem_kv.at[1]),
        )

    x_copy = pltpu.make_async_copy(xin_hbm, xin, sem_x)
    x_copy.start()
    for c in range(n_k):
        for cp in qkv_copies(0, c):
            cp.start()
    for cp in kv_copies(0):
        cp.start()
    wo_copy(0).start()
    for c in range(n_gk):
        wg_copy(0, c).start()
        wu_copy(0, c).start()
    wd_copy(0).start()

    barrier = pltpu.get_barrier_semaphore()
    for e in range(1, n_sp):
        pl.semaphore_signal(barrier, inc=1, device_id={"sp": lax.rem(s_idx + e, n_sp)}, device_id_type=MESH)
    for d in range(1, n_tp):
        pl.semaphore_signal(barrier, inc=1, device_id={"tp": lax.rem(i_idx + d, n_tp)}, device_id_type=MESH)

    def norm_block(load, store, gain_ref, l):
        total = None
        for c in range(n_tp):
            v = load(c).astype(F32)
            total = v * v if total is None else total + v * v
        mean_sq = jnp.sum(total, axis=-1, keepdims=True) * (1.0 / width)
        inv = lax.rsqrt(mean_sq + EPSILON)
        for c in range(n_tp):
            gain = gain_ref[pl.ds(l, 1), pl.ds(c * cols, cols)].astype(F32)
            store(c, (load(c).astype(F32) * inv * gain).astype(BF16))

    def project_qkv(l, h_ref, n_rows):
        qacc[pl.ds(0, n_rows), :] = jnp.zeros((n_rows, qacc.shape[1]), F32)

        @pl.loop(0, n_k)
        def _(c):
            for cp in qkv_copies(l, c):
                cp.wait()
            ks = pl.ds(pl.multiple_of(c * k_chunk, k_chunk), k_chunk)
            qacc[pl.ds(0, n_rows), :] += jnp.dot(h_ref[:, ks], wqkv[ks, :], preferred_element_type=F32)
            if l + 1 < n_layers:
                for cp in qkv_copies(l + 1, c):
                    cp.start()

    my_rows = pl.ds(pl.multiple_of(s_idx * rows, rows), rows)
    my_cols = pl.ds(pl.multiple_of(i_idx * cols, cols), cols)

    x_copy.wait()

    xres[...] = xin[my_rows, my_cols]

    @pl.loop(0, n_sp)
    def _(r):
        rs = pl.ds(pl.multiple_of(r * rows, rows), rows)

        def store(c, v):
            xin[rs, pl.ds(c * cols, cols)] = v

        norm_block(lambda c: xin[rs, pl.ds(c * cols, cols)], store, ga_ref, 0)

    pl.semaphore_wait(barrier, n_sp + n_tp - 2)

    def attention(l):
        qf = qkvf.at[l]
        for cp in kv_copies(l):
            cp.wait()

        @pl.loop(0, batch // sub)
        def _(gi):
            r0 = pl.multiple_of(gi * sub, sub)
            kk = qf[pl.ds(r0, sub), pl.ds(qw, head)].astype(F32)
            q64 = jnp.concatenate([qf[pl.ds(r0, sub), pl.ds(g * head, head)] for g in range(group)], axis=0)
            k16 = kbuf[pl.ds(pl.multiple_of(gi * sub * t_local, sub * t_local), sub * t_local), :]
            s4 = lax.dot_general(q64, k16, (((1,), (1,)), ((), ())), preferred_element_type=F32)
            which = lax.rem(lax.broadcasted_iota(jnp.int32, (group * sub, span), 0), sub) // 4
            comb = s4[:, 0:span]
            for j in range(1, sub // 4):
                comb = jnp.where(which == j, s4[:, j * span:(j + 1) * span], comb)
            o0 = pl.multiple_of(gi * group * sub, group * sub)
            sbuf[pl.ds(o0, group * sub), :] = comb * scale
            kt = jnp.concatenate([kk] * group, axis=0)
            snew[pl.ds(o0, group * sub), :] = jnp.sum(q64.astype(F32) * kt, axis=-1, keepdims=True) * scale

        @pl.loop(0, n_sp)
        def _(t):
            rs = pl.ds(pl.multiple_of(t * blk, blk), blk)
            row_b = lax.broadcasted_iota(jnp.int32, (blk, batch), 0)
            row_b = t * rows + (row_b // (group * sub)) * sub + lax.rem(row_b, sub)
            lane_b = lax.broadcasted_iota(jnp.int32, (blk, batch), 1)
            lens = len_ref[...].astype(F32)
            len_row = jnp.sum(jnp.where(row_b == lane_b, lens, 0.0), axis=1, keepdims=True)
            lane = lax.broadcasted_iota(jnp.int32, (blk, span), 1)
            row = lax.broadcasted_iota(jnp.int32, (blk, span), 0)
            pos = (lax.rem(lane, t_local) + s_idx * t_local).astype(F32)
            valid = jnp.logical_and(lane // t_local == lax.rem(row, 4), pos < len_row)
            sc = jnp.where(valid, sbuf[rs, :], NEG_BIG)
            top = jnp.maximum(jnp.max(sc, axis=-1, keepdims=True), snew[rs, :])
            prob = jnp.where(valid, jnp.exp(sc - top), 0.0)
            tot = jnp.sum(prob, axis=-1, keepdims=True)
            sbuf[rs, :] = prob
            eye = lax.broadcasted_iota(jnp.int32, (blk, blk), 0) == lax.broadcasted_iota(jnp.int32, (blk, blk), 1)
            stsend[t, pl.ds(0, 1), :] = jnp.sum(jnp.where(eye, top, 0.0), axis=0, keepdims=True)
            stsend[t, pl.ds(1, 1), :] = jnp.sum(jnp.where(eye, tot, 0.0), axis=0, keepdims=True)

        @pl.loop(0, batch // sub)
        def _(gi):
            o0 = pl.multiple_of(gi * group * sub, group * sub)
            pr = sbuf[pl.ds(o0, group * sub), :]
            which = lax.rem(lax.broadcasted_iota(jnp.int32, (group * sub, span), 0), sub) // 4
            wide = jnp.concatenate([jnp.where(which == j, pr, 0.0).astype(BF16) for j in range(sub // 4)], axis=1)
            v16 = vbuf[pl.ds(pl.multiple_of(gi * sub * t_local, sub * t_local), sub * t_local), :]
            obuf[pl.ds(o0, group * sub), :] = jnp.dot(wide, v16, preferred_element_type=F32).astype(BF16)

        if l + 1 < n_layers:
            for cp in kv_copies(l + 1):
                cp.start()

    def combine_over_sp(l):
        sends = []
        for e in range(1, n_sp):
            t = lax.rem(s_idx + e, n_sp)
            rs = pl.ds(pl.multiple_of(t * blk, blk), blk)
            a = pltpu.make_async_remote_copy(
                src_ref=stsend.at[t], dst_ref=strecv.at[e - 1], send_sem=yt_send.at[e - 1],
                recv_sem=yt_recv.at[e - 1], device_id={"sp": t}, device_id_type=MESH)
            b = pltpu.make_async_remote_copy(
                src_ref=obuf.at[rs, :], dst_ref=orecv.at[e - 1], send_sem=ys_send.at[e - 1],
                recv_sem=ys_recv.at[e - 1], device_id={"sp": t}, device_id_type=MESH)
            a.start()
            b.start()
            sends += [a, b]
        eye = lax.broadcasted_iota(jnp.int32, (blk, blk), 0) == lax.broadcasted_iota(jnp.int32, (blk, blk), 1)

        def column(v):
            return jnp.sum(jnp.where(eye, v, 0.0), axis=1, keepdims=True)

        my_blk = pl.ds(pl.multiple_of(s_idx * blk, blk), blk)
        sn = snew[my_blk, :]
        for cp in sends:
            cp.wait()
        tops = [column(stsend[s_idx, pl.ds(0, 1), :])] + [column(strecv[e, pl.ds(0, 1), :]) for e in range(n_sp - 1)]
        tots = [column(stsend[s_idx, pl.ds(1, 1), :])] + [column(strecv[e, pl.ds(1, 1), :]) for e in range(n_sp - 1)]
        run_max = sn
        for m in tops:
            run_max = jnp.maximum(run_max, m)
        p_new = jnp.exp(sn - run_max)
        denom = p_new
        v_own = qkvf[l, my_rows, pl.ds(qw + head, head)].astype(F32)
        v_rows = jnp.concatenate([v_own[b * sub:(b + 1) * sub] for b in range(rows // sub) for _ in range(group)], axis=0)
        numer = p_new.astype(BF16).astype(F32) * v_rows
        parts = [obuf[my_blk, :]] + [orecv[e] for e in range(n_sp - 1)]
        for m, tt, o in zip(tops, tots, parts):
            w = jnp.exp(m - run_max)
            denom = denom + w * tt
            numer = numer + w * o.astype(F32)
        res = (numer / denom).astype(BF16)
        for b in range(rows // sub):
            for g in range(group):
                a0 = (b * group + g) * sub
                o2d[pl.ds(b * sub, sub), pl.ds(g * head, head)] = res[a0:a0 + sub, :]

    def rs_copy(d, j):
        return pltpu.make_async_remote_copy(
            src_ref=psend.at[d], dst_ref=precv.at[d], send_sem=rs_send.at[d], recv_sem=rs_recv.at[d],
            device_id={"tp": j}, device_id_type=MESH)

    def reduce_over_tp(lhs_ref, w_ref, step):
        @pl.loop(0, n_tp // step)
        def _(it):
            for u in range(step):
                d = it * step + u
                j = lax.rem(i_idx + 1 + d, n_tp)
                part = jnp.dot(lhs_ref[...], w_ref[:, pl.ds(pl.multiple_of(j * cols, cols), cols)],
                               preferred_element_type=F32)
                if u < step - 1:
                    psend[d] = part.astype(BF16)
                    rs_copy(d, j).start()
                else:
                    @pl.when(d < n_tp - 1)
                    def _():
                        psend[d] = part.astype(BF16)
                        rs_copy(d, j).start()

                    @pl.when(d == n_tp - 1)
                    def _():
                        prev[...] = part

        acc = prev[...]
        for d in range(n_tp - 1):
            rs_copy(d, lax.rem(i_idx + 1 + d, n_tp)).wait()
            acc = acc + precv[d].astype(F32)
        xres[...] = (xres[...].astype(F32) + acc).astype(BF16)

    def ag_copy(d):
        return pltpu.make_async_remote_copy(
            src_ref=xres, dst_ref=xbuf.at[i_idx], send_sem=ag_send.at[d], recv_sem=ag_recv.at[d],
            device_id={"tp": lax.rem(i_idx + 1 + d, n_tp)}, device_id_type=MESH)

    def gather_and_norm(gain_ref, l):
        for d in range(n_tp - 1):
            ag_copy(d).start()
        xbuf[i_idx] = xres[...]
        for d in range(n_tp - 1):
            ag_copy(d).wait()

        def store(c, v):
            hrow[:, pl.ds(c * cols, cols)] = v

        norm_block(lambda c: xbuf[c], store, gain_ref, l)

    for l in range(n_layers):
        if l == 0:
            project_qkv(l, xin, batch)
            qkvf[l] = qacc[...].astype(BF16)
        else:
            gather_and_norm(ga_ref, l)
            project_qkv(l, hrow, rows)
            qkvf[l, my_rows, :] = qacc[pl.ds(0, rows), :].astype(BF16)
            copies = []
            for e in range(1, n_sp):
                cp = pltpu.make_async_remote_copy(
                    src_ref=qkvf.at[l, my_rows, :], dst_ref=qkvf.at[l, my_rows, :], send_sem=yq_send.at[e - 1],
                    recv_sem=yq_recv.at[e - 1], device_id={"sp": lax.rem(s_idx + e, n_sp)}, device_id_type=MESH)
                cp.start()
                copies.append(cp)
            for cp in copies:
                cp.wait()
        kn_ref[l] = qkvf[l, :, pl.ds(qw, head)]
        vn_ref[l] = qkvf[l, :, pl.ds(qw + head, head)]
        attention(l)
        combine_over_sp(l)
        wo_copy(l).wait()
        reduce_over_tp(o2d, wo, n_tp // 2)
        if l + 1 < n_layers:
            wo_copy(l + 1).start()
        gather_and_norm(gm_ref, l)
        gacc[...] = jnp.zeros(gacc.shape, F32)
        uacc[...] = jnp.zeros(uacc.shape, F32)

        @pl.loop(0, n_gk)
        def _(c):
            wg_copy(l, c).wait()
            wu_copy(l, c).wait()
            hk = hrow[:, pl.ds(pl.multiple_of(c * g_chunk, g_chunk), g_chunk)]
            gacc[...] += jnp.dot(hk, wg[c], preferred_element_type=F32)
            uacc[...] += jnp.dot(hk, wu[c], preferred_element_type=F32)
            if l + 1 < n_layers:
                wg_copy(l + 1, c).start()
                wu_copy(l + 1, c).start()

        act[...] = (jax.nn.silu(gacc[...]) * uacc[...]).astype(BF16)
        wd_copy(l).wait()
        reduce_over_tp(act, wd, 2)
        if l + 1 < n_layers:
            wd_copy(l + 1).start()

    xo_ref[my_rows, my_cols] = xres[...]
    f1 = []
    for e in range(1, n_sp):
        cp = pltpu.make_async_remote_copy(
            src_ref=xres, dst_ref=xo_ref.at[my_rows, my_cols], send_sem=f1_send.at[e - 1], recv_sem=f1_recv.at[e - 1],
            device_id={"sp": lax.rem(s_idx + e, n_sp)}, device_id_type=MESH)
        cp.start()
        f1.append(cp)
    for cp in f1:
        cp.wait()

    def strip(j):
        return xo_ref.at[:, pl.ds(pl.multiple_of(j * cols, cols), cols)]

    f2 = []
    for d in range(1, n_tp // 2):
        cp = pltpu.make_async_remote_copy(
            src_ref=strip(i_idx), dst_ref=strip(i_idx), send_sem=f2_send.at[d - 1], recv_sem=f2_recv.at[d - 1],
            device_id={"tp": lax.rem(i_idx + 2 * d, n_tp)}, device_id_type=MESH)
        cp.start()
        f2.append(cp)
    partner = i_idx + 1 - 2 * lax.rem(i_idx, 2)
    f3 = []
    for d in range(n_tp // 2):
        if d > 0:
            f2[d - 1].wait()
        j = lax.rem(i_idx + n_tp - 2 * d, n_tp)
        cp = pltpu.make_async_remote_copy(
            src_ref=strip(j), dst_ref=strip(j), send_sem=f3_send.at[d], recv_sem=f3_recv.at[d],
            device_id={"tp": partner}, device_id_type=MESH)
        cp.start()
        f3.append(cp)
    for cp in f3:
        cp.wait()


def solution(mesh):
    weight_col = P(None, None, "tp")
    weight_row = P(None, "tp", None)
    cache_spec = P(None, "dp", "tp", "sp", None)
    new_spec = P(None, "dp", "tp", None)
    n_sp = mesh.shape["sp"]
    n_tp = mesh.shape["tp"]

    def device_step(x_in, lengths, w_q, w_k, w_v, w_o, w_gate, w_up, w_down, gain_attn, gain_mlp, k_cache, v_cache):
        n_layers, width, qw = w_q.shape
        batch = x_in.shape[0]
        t_local, head = k_cache.shape[3], k_cache.shape[4]
        ff = w_gate.shape[2]
        group = qw // head
        rows, cols = batch // n_sp, width // n_tp
        n_k, n_gk = 4, 4
        kc = k_cache.reshape(n_layers, batch * t_local, head)
        vc = v_cache.reshape(n_layers, batch * t_local, head)
        vm = pl.BlockSpec(memory_space=pltpu.VMEM)
        hbm = pl.BlockSpec(memory_space=pl.ANY)
        dma = pltpu.SemaphoreType.DMA
        scratch = [
            pltpu.VMEM((width, qw + 2 * head), BF16),
            pltpu.VMEM((qw, width), BF16),
            pltpu.VMEM((n_gk, width // n_gk, ff), BF16),
            pltpu.VMEM((n_gk, width // n_gk, ff), BF16),
            pltpu.VMEM((ff, width), BF16),
            pltpu.VMEM((batch * t_local, head), BF16),
            pltpu.VMEM((batch * t_local, head), BF16),
            pltpu.VMEM((batch, width), BF16),
            pltpu.VMEM((rows, width), BF16),
            pltpu.VMEM((n_layers, batch, qw + 2 * head), BF16),
            pltpu.VMEM((batch, qw + 2 * head), F32),
            pltpu.VMEM((batch * group, 1), F32),
            pltpu.VMEM((batch * group, 4 * t_local), F32),
            pltpu.VMEM((batch * group, head), BF16),
            pltpu.VMEM((n_sp, 8, rows * group), F32),
            pltpu.VMEM((n_sp - 1, rows * group, head), BF16),
            pltpu.VMEM((n_sp - 1, 8, rows * group), F32),
            pltpu.VMEM((rows, qw), BF16),
            pltpu.VMEM((rows, ff), F32),
            pltpu.VMEM((rows, ff), F32),
            pltpu.VMEM((rows, ff), BF16),
            pltpu.VMEM((n_tp - 1, rows, cols), BF16),
            pltpu.VMEM((rows, cols), F32),
            pltpu.VMEM((n_tp - 1, rows, cols), BF16),
            pltpu.VMEM((rows, cols), BF16),
            pltpu.VMEM((n_tp, rows, cols), BF16),
            dma, dma((n_k, 3)), dma, dma((n_gk,)), dma((n_gk,)), dma, dma((2,)),
        ]
        scratch += [dma((n_sp - 1,))] * 6 + [dma((n_tp - 1,))] * 4
        scratch += [dma((n_sp - 1,))] * 2 + [dma((n_tp // 2 - 1,))] * 2 + [dma((n_tp // 2,))] * 2
        x_out, k_new, v_new = pl.pallas_call(
            functools.partial(decode_kernel, n_sp, n_tp),
            out_shape=(
                jax.ShapeDtypeStruct((batch, width), BF16),
                jax.ShapeDtypeStruct((n_layers, batch, head), BF16),
                jax.ShapeDtypeStruct((n_layers, batch, head), BF16),
            ),
            in_specs=[vm, hbm, hbm, hbm, hbm, hbm, hbm, hbm, hbm, vm, vm, hbm, hbm],
            out_specs=(vm, vm, vm),
            scratch_shapes=scratch,
            compiler_params=pltpu.CompilerParams(collective_id=0, has_side_effects=True, vmem_limit_bytes=VMEM_LIMIT),
            name="decode_layers",
        )(lengths.reshape(1, batch), x_in, w_q, w_k, w_v, w_o, w_gate, w_up, w_down, gain_attn, gain_mlp, kc, vc)
        return x_out, k_new.reshape(n_layers, batch, 1, head), v_new.reshape(n_layers, batch, 1, head)

    in_specs = (P("dp", None), P("dp"), weight_col, weight_col, weight_col, weight_row, weight_col, weight_col, weight_row, P(None, None), P(None, None), cache_spec, cache_spec)
    out_specs = (P("dp", None), new_spec, new_spec)
    return jax.shard_map(device_step, mesh=mesh, in_specs=in_specs, out_specs=out_specs, check_vma=False)
```

```python
import functools
import itertools

import jax
import jax.numpy as jnp
from jax import lax
from jax.experimental import pallas as pl
from jax.experimental.pallas import tpu as pltpu
from jax.sharding import PartitionSpec as P

EPSILON = 1e-5
NEG_BIG = -1e30
F32 = jnp.float32
BF16 = jnp.bfloat16
MESH = pl.DeviceIdType.MESH
VMEM_LIMIT = 64487424


def decode_kernel(
    n_sp, n_tp,
    len_ref, xin_hbm, wq_hbm, wk_hbm, wv_hbm, wo_hbm, wg_hbm, wu_hbm, wd_hbm, ga_ref, gm_ref, kc_hbm, vc_hbm,
    xo_ref, kn_ref, vn_ref,
    wqkv, wo, wg, wu, wd, kbuf, vbuf, xin, hrow, qkvf, qacc, snew, obuf, stsend, orecv, strecv, o2d,
    gacc, uacc, act, psend, prev, precv, xres, xbuf,
    sem_x, sem_qkv, sem_wo, sem_wg, sem_wu, sem_wd, sem_kv,
    ys_send, ys_recv, yt_send, yt_recv, yq_send, yq_recv,
    rs_send, rs_recv, ag_send, ag_recv,
    f1_send, f1_recv, f2_send, f2_recv, f3_send, f3_recv,
):
    scope = jax.named_scope
    n_layers = wq_hbm.shape[0]
    batch, width = xin.shape
    head = kbuf.shape[1]
    qw = wq_hbm.shape[2]
    group = qw // head
    t_local = kbuf.shape[0] // batch
    rows = batch // n_sp
    cols = width // n_tp
    n_k = sem_qkv.shape[0]
    k_chunk = width // n_k
    n_gk = wg.shape[0]
    g_chunk = wg.shape[1]
    scale = head ** -0.5
    blk = rows * group
    sub = 16
    span = 4 * t_local
    s_idx = lax.axis_index("sp")
    i_idx = lax.axis_index("tp")

    def tp_peer(d):
        return lax.rem(i_idx + tp_offset(d), n_tp)

    def tp_offset(d):
        turn = (d + 1) // 2
        return (n_tp // 2 + turn - 2 * turn * (d % 2)) % n_tp

    def qkv_copies(l, c):
        ks = pl.ds(c * k_chunk, k_chunk)
        return (
            pltpu.make_async_copy(wq_hbm.at[l, ks, :], wqkv.at[ks, pl.ds(0, qw)], sem_qkv.at[c, 0]),
            pltpu.make_async_copy(wk_hbm.at[l, ks, :], wqkv.at[ks, pl.ds(qw, head)], sem_qkv.at[c, 1]),
            pltpu.make_async_copy(wv_hbm.at[l, ks, :], wqkv.at[ks, pl.ds(qw + head, head)], sem_qkv.at[c, 2]),
        )

    def wo_copy(l):
        return pltpu.make_async_copy(wo_hbm.at[l], wo, sem_wo)

    def wg_copy(l, c):
        return pltpu.make_async_copy(wg_hbm.at[l, pl.ds(c * g_chunk, g_chunk), :], wg.at[c], sem_wg.at[c])

    def wu_copy(l, c):
        return pltpu.make_async_copy(wu_hbm.at[l, pl.ds(c * g_chunk, g_chunk), :], wu.at[c], sem_wu.at[c])

    def wd_copy(l):
        return pltpu.make_async_copy(wd_hbm.at[l], wd, sem_wd)

    def kv_copies(l):
        return (
            pltpu.make_async_copy(kc_hbm.at[l], kbuf, sem_kv.at[0]),
            pltpu.make_async_copy(vc_hbm.at[l], vbuf, sem_kv.at[1]),
        )

    x_copy = pltpu.make_async_copy(xin_hbm, xin, sem_x)
    x_copy.start()

    barrier = pltpu.get_barrier_semaphore()
    for e in range(1, n_sp):
        pl.semaphore_signal(barrier, inc=1, device_id={"sp": lax.rem(s_idx + e, n_sp)}, device_id_type=MESH)
    for d in range(1, n_tp):
        pl.semaphore_signal(barrier, inc=1, device_id={"tp": lax.rem(i_idx + d, n_tp)}, device_id_type=MESH)

    def norm_block(load, store, gain_ref, l):
        total = None
        for c in range(n_tp):
            v = load(c).astype(F32)
            total = v * v if total is None else total + v * v
        mean_sq = jnp.sum(total, axis=-1, keepdims=True) * (1.0 / width)
        inv = lax.rsqrt(mean_sq + EPSILON)
        for c in range(n_tp):
            gain = gain_ref[pl.ds(l, 1), pl.ds(c * cols, cols)].astype(F32)
            store(c, (load(c).astype(F32) * inv * gain).astype(BF16))

    def project_qkv(l, h_ref, n_rows):
        qacc[pl.ds(0, n_rows), :] = jnp.zeros((n_rows, qacc.shape[1]), F32)

        @pl.loop(0, n_k)
        def _(c):
            for cp in qkv_copies(l, c):
                cp.wait()
            ks = pl.ds(pl.multiple_of(c * k_chunk, k_chunk), k_chunk)
            qacc[pl.ds(0, n_rows), :] += jnp.dot(h_ref[:, ks], wqkv[ks, :], preferred_element_type=F32)
            if l + 1 < n_layers:
                for cp in qkv_copies(l + 1, c):
                    cp.start()

    my_rows = pl.ds(pl.multiple_of(s_idx * rows, rows), rows)
    my_cols = pl.ds(pl.multiple_of(i_idx * cols, cols), cols)

    with scope("x_wait"):
        x_copy.wait()
    for c in range(n_k):
        for cp in qkv_copies(0, c):
            cp.start()
    for cp in kv_copies(0):
        cp.start()
    wo_copy(0).start()

    xres[...] = xin[my_rows, my_cols]

    with scope("norm"):
        @pl.loop(0, n_sp)
        def _(r):
            rs = pl.ds(pl.multiple_of(r * rows, rows), rows)

            def store(c, v):
                xin[rs, pl.ds(c * cols, cols)] = v

            norm_block(lambda c: xin[rs, pl.ds(c * cols, cols)], store, ga_ref, 0)


    def sp_copies(e):
        t = lax.rem(s_idx + e, n_sp)
        return (
            pltpu.make_async_remote_copy(
                src_ref=stsend.at[t], dst_ref=strecv.at[e - 1], send_sem=yt_send.at[e - 1],
                recv_sem=yt_recv.at[e - 1], device_id={"sp": t}, device_id_type=MESH),
            pltpu.make_async_remote_copy(
                src_ref=obuf.at[t], dst_ref=orecv.at[e - 1], send_sem=ys_send.at[e - 1],
                recv_sem=ys_recv.at[e - 1], device_id={"sp": t}, device_id_type=MESH),
        )

    def qkv_copy(l, e):
        return pltpu.make_async_remote_copy(
            src_ref=qkvf.at[l, my_rows, :], dst_ref=qkvf.at[l, my_rows, :], send_sem=yq_send.at[e - 1],
            recv_sem=yq_recv.at[e - 1], device_id={"sp": lax.rem(s_idx + e, n_sp)}, device_id_type=MESH)

    n_sub = rows // sub
    tall = group * sub
    which = lax.rem(lax.broadcasted_iota(jnp.int32, (tall, span), 0), sub) // 4
    eye = lax.broadcasted_iota(jnp.int32, (blk, blk), 0) == lax.broadcasted_iota(jnp.int32, (blk, blk), 1)

    def attend(l, t):
        scores, news = [], []
        for u in range(n_sub):
            r0 = pl.multiple_of(t * rows + u * sub, sub)
            kk = qkvf[l, pl.ds(r0, sub), pl.ds(qw, head)].astype(F32)
            q64 = jnp.concatenate([qkvf[l, pl.ds(r0, sub), pl.ds(g * head, head)] for g in range(group)], axis=0)
            k16 = kbuf[pl.ds(pl.multiple_of(r0 * t_local, sub * t_local), sub * t_local), :]
            s4 = lax.dot_general(q64, k16, (((1,), (1,)), ((), ())), preferred_element_type=F32)
            comb = s4[:, 0:span]
            for j in range(1, sub // 4):
                comb = jnp.where(which == j, s4[:, j * span:(j + 1) * span], comb)
            scores.append(comb * scale)
            kt = jnp.concatenate([kk] * group, axis=0)
            news.append(jnp.sum(q64.astype(F32) * kt, axis=-1, keepdims=True) * scale)
        score = jnp.concatenate(scores, axis=0)
        s_new = jnp.concatenate(news, axis=0)
        row_b = lax.broadcasted_iota(jnp.int32, (blk, batch), 0)
        row_b = t * rows + (row_b // tall) * sub + lax.rem(row_b, sub)
        lane_b = lax.broadcasted_iota(jnp.int32, (blk, batch), 1)
        lens = len_ref[...].astype(F32)
        len_row = jnp.sum(jnp.where(row_b == lane_b, lens, 0.0), axis=1, keepdims=True)
        lane = lax.broadcasted_iota(jnp.int32, (blk, span), 1)
        row = lax.broadcasted_iota(jnp.int32, (blk, span), 0)
        pos = (lax.rem(lane, t_local) + s_idx * t_local).astype(F32)
        valid = jnp.logical_and(lane // t_local == lax.rem(row, 4), pos < len_row)
        score = jnp.where(valid, score, NEG_BIG)
        top = jnp.maximum(jnp.max(score, axis=-1, keepdims=True), s_new)
        prob = jnp.where(valid, jnp.exp(score - top), 0.0)
        tot = jnp.sum(prob, axis=-1, keepdims=True)
        stsend[t, pl.ds(0, 1), :] = jnp.sum(jnp.where(eye, top, 0.0), axis=0, keepdims=True)
        stsend[t, pl.ds(1, 1), :] = jnp.sum(jnp.where(eye, tot, 0.0), axis=0, keepdims=True)
        for u in range(n_sub):
            pr = prob[u * tall:(u + 1) * tall]
            wide = jnp.concatenate([jnp.where(which == j, pr, 0.0).astype(BF16) for j in range(sub // 4)], axis=1)
            v0 = pl.multiple_of((t * rows + u * sub) * t_local, sub * t_local)
            obuf[t, pl.ds(u * tall, tall), :] = jnp.dot(
                wide, vbuf[pl.ds(v0, sub * t_local), :], preferred_element_type=F32).astype(BF16)
        return s_new

    def attention(l):
        for cp in kv_copies(l):
            cp.wait()
        order = (2, 1, 3, 0) if l == 0 else (0, 1, 3, 2)
        for e in order:
            if l > 0 and e > 0:
                qkv_copy(l, n_sp - e).wait()
            out = attend(l, lax.rem(s_idx + e, n_sp))
            if l == 0 and e == order[0]:
                pl.semaphore_wait(barrier, n_sp + n_tp - 2)
            if e == 0:
                snew[...] = out
            else:
                for cp in sp_copies(e):
                    cp.start()
        if l + 1 < n_layers:
            for cp in kv_copies(l + 1):
                cp.start()

    def combine_over_sp(l):
        def column(v):
            return jnp.sum(jnp.where(eye, v, 0.0), axis=1, keepdims=True)

        sn = snew[...]
        tops = [column(stsend[s_idx, pl.ds(0, 1), :])]
        tots = [column(stsend[s_idx, pl.ds(1, 1), :])]
        parts = [obuf[s_idx]]
        with scope("sp_wait"):
            for e in range(1, n_sp):
                for cp in sp_copies(e):
                    cp.wait()
        for e in range(1, n_sp):
            tops.append(column(strecv[e - 1, pl.ds(0, 1), :]))
            tots.append(column(strecv[e - 1, pl.ds(1, 1), :]))
            parts.append(orecv[e - 1])
        run_max = sn
        for m in tops:
            run_max = jnp.maximum(run_max, m)
        p_new = jnp.exp(sn - run_max)
        denom = p_new
        v_own = qkvf[l, my_rows, pl.ds(qw + head, head)].astype(F32)
        v_rows = jnp.concatenate([v_own[b * sub:(b + 1) * sub] for b in range(n_sub) for _ in range(group)], axis=0)
        numer = p_new.astype(BF16).astype(F32) * v_rows
        for m, tt, o in zip(tops, tots, parts):
            w = jnp.exp(m - run_max)
            denom = denom + w * tt
            numer = numer + w * o.astype(F32)
        res = (numer / denom).astype(BF16)
        for b in range(n_sub):
            for g in range(group):
                a0 = (b * group + g) * sub
                o2d[pl.ds(b * sub, sub), pl.ds(g * head, head)] = res[a0:a0 + sub, :]

    def rs_copy(d, j):
        return pltpu.make_async_remote_copy(
            src_ref=psend.at[d], dst_ref=precv.at[d], send_sem=rs_send.at[d], recv_sem=rs_recv.at[d],
            device_id={"tp": j}, device_id_type=MESH)

    def reduce_over_tp(lhs_ref, w_ref, step):
        @pl.loop(0, n_tp // step)
        def _(it):
            for u in range(step):
                d = it * step + u
                j = tp_peer(d)
                part = jnp.dot(lhs_ref[...], w_ref[:, pl.ds(pl.multiple_of(j * cols, cols), cols)],
                               preferred_element_type=F32)
                if u < step - 1:
                    psend[d] = part.astype(BF16)
                    rs_copy(d, j).start()
                else:
                    @pl.when(d < n_tp - 1)
                    def _():
                        psend[d] = part.astype(BF16)
                        rs_copy(d, j).start()

                    @pl.when(d == n_tp - 1)
                    def _():
                        prev[...] = part

        with scope("reduce"):
            acc = prev[...]
            for d in range(n_tp - 1):
                rs_copy(d, tp_peer(d)).wait()
                acc = acc + precv[d].astype(F32)
        xres[...] = (xres[...].astype(F32) + acc).astype(BF16)

    def ag_copy(d):
        return pltpu.make_async_remote_copy(
            src_ref=xres, dst_ref=xbuf.at[i_idx], send_sem=ag_send.at[d], recv_sem=ag_recv.at[d],
            device_id={"tp": tp_peer(d)}, device_id_type=MESH)

    def gather_and_norm(gain_ref, l):
        for d in range(n_tp - 1):
            ag_copy(d).start()
        xbuf[i_idx] = xres[...]
        for d in range(n_tp - 1):
            ag_copy(d).wait()

        def store(c, v):
            hrow[:, pl.ds(c * cols, cols)] = v

        with scope("norm"):
            norm_block(lambda c: xbuf[c], store, gain_ref, l)

    for l in range(n_layers):
        if l == 0:
            with scope("qkv"):
                project_qkv(l, xin, batch)
                qkvf[l] = qacc[...].astype(BF16)
            for c in range(n_gk):
                wg_copy(0, c).start()
                wu_copy(0, c).start()
        else:
            with scope("gather_a"):
                gather_and_norm(ga_ref, l)
            with scope("qkv"):
                project_qkv(l, hrow, rows)
                qkvf[l, my_rows, :] = qacc[pl.ds(0, rows), :].astype(BF16)
            for e in (2, 1, 3):
                qkv_copy(l, e).start()
        with scope("attention"):
            attention(l)
        kn_ref[l] = qkvf[l, :, pl.ds(qw, head)]
        vn_ref[l] = qkvf[l, :, pl.ds(qw + head, head)]
        if l == 0:
            wd_copy(0).start()
        with scope("combine"):
            combine_over_sp(l)
        with scope("wo"):
            wo_copy(l).wait()
            reduce_over_tp(o2d, wo, n_tp // 2)
        if l + 1 < n_layers:
            wo_copy(l + 1).start()
        with scope("gather_m"):
            gather_and_norm(gm_ref, l)
        with scope("gate_up"):
            gacc[...] = jnp.zeros(gacc.shape, F32)
            uacc[...] = jnp.zeros(uacc.shape, F32)

            @pl.loop(0, n_gk)
            def _(c):
                wg_copy(l, c).wait()
                wu_copy(l, c).wait()
                hk = hrow[:, pl.ds(pl.multiple_of(c * g_chunk, g_chunk), g_chunk)]
                gacc[...] += jnp.dot(hk, wg[c], preferred_element_type=F32)
                uacc[...] += jnp.dot(hk, wu[c], preferred_element_type=F32)
                if l + 1 < n_layers:
                    wg_copy(l + 1, c).start()
                    wu_copy(l + 1, c).start()

            act[...] = (jax.nn.silu(gacc[...]) * uacc[...]).astype(BF16)
        with scope("down"):
            wd_copy(l).wait()
            reduce_over_tp(act, wd, 2)
        if l + 1 < n_layers:
            wd_copy(l + 1).start()

    n_x = n_tp // 2
    half = rows // 2
    partner = i_idx + 1 - 2 * lax.rem(i_idx, 2)

    def block(e, d, r0, n):
        t = lax.rem(s_idx + n_sp - e, n_sp)
        j = lax.rem(i_idx + n_tp - 2 * d, n_tp)
        return xo_ref.at[pl.ds(pl.multiple_of(t * rows + r0, half), n), pl.ds(pl.multiple_of(j * cols, cols), cols)]

    def send_sp(ref, e, k):
        return pltpu.make_async_remote_copy(
            src_ref=ref, dst_ref=ref, send_sem=f1_send.at[k], recv_sem=f1_recv.at[k],
            device_id={"sp": lax.rem(s_idx + e, n_sp)}, device_id_type=MESH)

    def send_x(ref, d, k):
        return pltpu.make_async_remote_copy(
            src_ref=ref, dst_ref=ref, send_sem=f2_send.at[k], recv_sem=f2_recv.at[k],
            device_id={"tp": lax.rem(i_idx + 2 * d, n_tp)}, device_id_type=MESH)

    def send_core(ref, k):
        return pltpu.make_async_remote_copy(
            src_ref=ref, dst_ref=ref, send_sem=f3_send.at[k], recv_sem=f3_recv.at[k],
            device_id={"tp": partner}, device_id_type=MESH)

    sent = []

    def go(cp):
        cp.start()
        sent.append(cp)

    with scope("final"):
        xo_ref[my_rows, my_cols] = xres[...]
        far_sp = sorted(range(1, n_sp), key=lambda e: -min(e, n_sp - e))
        far_x = sorted(range(1, n_x), key=lambda d: -min(d, n_x - d))
        for e, d in itertools.zip_longest(far_sp, far_x):
            if e is not None:
                go(send_sp(block(0, 0, 0, rows), e, e - 1))
            if d is not None:
                go(send_x(block(0, 0, 0, rows), d, d - 1))
        core = []

        def to_core(ref):
            cp = send_core(ref, len(core))
            core.append(cp)
            go(cp)

        to_core(block(0, 0, 0, rows))
        for e, d in itertools.zip_longest(far_sp[::-1], far_x[::-1]):
            if e is not None:
                ref = block(e, 0, 0, rows)
                send_sp(ref, e, e - 1).wait_recv()
                for d2 in far_x:
                    go(send_x(block(e, 0, 0, half), d2, (n_x - 1) * e + d2 - 1))
                to_core(ref)
            if d is not None:
                ref = block(0, d, 0, rows)
                send_x(ref, d, d - 1).wait_recv()
                for e2 in far_sp:
                    go(send_sp(block(0, d, half, half), e2, (n_sp - 1) * d + e2 - 1))
                to_core(ref)
        for e in far_sp[::-1]:
            for d in far_x[::-1]:
                ref = block(e, d, 0, half)
                send_x(ref, d, (n_x - 1) * e + d - 1).wait_recv()
                to_core(ref)
                ref = block(e, d, half, half)
                send_sp(ref, e, (n_sp - 1) * d + e - 1).wait_recv()
                to_core(ref)
        for cp in core:
            cp.wait_recv()
        for cp in sent:
            cp.wait_send()


def solution(mesh):
    weight_col = P(None, None, "tp")
    weight_row = P(None, "tp", None)
    cache_spec = P(None, "dp", "tp", "sp", None)
    new_spec = P(None, "dp", "tp", None)
    n_sp = mesh.shape["sp"]
    n_tp = mesh.shape["tp"]

    def device_step(x_in, lengths, w_q, w_k, w_v, w_o, w_gate, w_up, w_down, gain_attn, gain_mlp, k_cache, v_cache):
        n_layers, width, qw = w_q.shape
        batch = x_in.shape[0]
        t_local, head = k_cache.shape[3], k_cache.shape[4]
        ff = w_gate.shape[2]
        group = qw // head
        rows, cols = batch // n_sp, width // n_tp
        n_k, n_gk = 4, 4
        kc = k_cache.reshape(n_layers, batch * t_local, head)
        vc = v_cache.reshape(n_layers, batch * t_local, head)
        vm = pl.BlockSpec(memory_space=pltpu.VMEM)
        hbm = pl.BlockSpec(memory_space=pl.ANY)
        dma = pltpu.SemaphoreType.DMA
        scratch = [
            pltpu.VMEM((width, qw + 2 * head), BF16),
            pltpu.VMEM((qw, width), BF16),
            pltpu.VMEM((n_gk, width // n_gk, ff), BF16),
            pltpu.VMEM((n_gk, width // n_gk, ff), BF16),
            pltpu.VMEM((ff, width), BF16),
            pltpu.VMEM((batch * t_local, head), BF16),
            pltpu.VMEM((batch * t_local, head), BF16),
            pltpu.VMEM((batch, width), BF16),
            pltpu.VMEM((rows, width), BF16),
            pltpu.VMEM((n_layers, batch, qw + 2 * head), BF16),
            pltpu.VMEM((batch, qw + 2 * head), F32),
            pltpu.VMEM((rows * group, 1), F32),
            pltpu.VMEM((n_sp, rows * group, head), BF16),
            pltpu.VMEM((n_sp, 8, rows * group), F32),
            pltpu.VMEM((n_sp - 1, rows * group, head), BF16),
            pltpu.VMEM((n_sp - 1, 8, rows * group), F32),
            pltpu.VMEM((rows, qw), BF16),
            pltpu.VMEM((rows, ff), F32),
            pltpu.VMEM((rows, ff), F32),
            pltpu.VMEM((rows, ff), BF16),
            pltpu.VMEM((n_tp - 1, rows, cols), BF16),
            pltpu.VMEM((rows, cols), F32),
            pltpu.VMEM((n_tp - 1, rows, cols), BF16),
            pltpu.VMEM((rows, cols), BF16),
            pltpu.VMEM((n_tp, rows, cols), BF16),
            dma, dma((n_k, 3)), dma, dma((n_gk,)), dma((n_gk,)), dma, dma((2,)),
        ]
        scratch += [dma((n_sp - 1,))] * 6 + [dma((n_tp - 1,))] * 4
        n_x = n_tp // 2
        scratch += [dma(((n_sp - 1) * n_x,))] * 2 + [dma(((n_x - 1) * n_sp,))] * 2 + [dma((2 * n_sp * n_x - n_sp - n_x + 1,))] * 2
        x_out, k_new, v_new = pl.pallas_call(
            functools.partial(decode_kernel, n_sp, n_tp),
            out_shape=(
                pltpu.VMEM((batch, width), BF16),
                pltpu.VMEM((n_layers, batch, head), BF16),
                pltpu.VMEM((n_layers, batch, head), BF16),
            ),
            in_specs=[vm, hbm, hbm, hbm, hbm, hbm, hbm, hbm, hbm, vm, vm, hbm, hbm],
            out_specs=(vm, vm, vm),
            scratch_shapes=scratch,
            compiler_params=pltpu.CompilerParams(collective_id=0, has_side_effects=True, vmem_limit_bytes=VMEM_LIMIT),
            name="decode_layers",
        )(lengths.reshape(1, batch), x_in, w_q, w_k, w_v, w_o, w_gate, w_up, w_down, gain_attn, gain_mlp, kc, vc)
        return x_out, k_new.reshape(n_layers, batch, 1, head), v_new.reshape(n_layers, batch, 1, head)

    in_specs = (P("dp", None), P("dp"), weight_col, weight_col, weight_col, weight_row, weight_col, weight_col, weight_row, P(None, None), P(None, None), cache_spec, cache_spec)
    out_specs = (P("dp", None), new_spec, new_spec)
    return jax.shard_map(device_step, mesh=mesh, in_specs=in_specs, out_specs=out_specs, check_vma=False)
```

```python
import functools
import itertools

import jax
import jax.numpy as jnp
from jax import lax
from jax.experimental import pallas as pl
from jax.experimental.pallas import tpu as pltpu
from jax.sharding import PartitionSpec as P

EPSILON = 1e-5
NEG_BIG = -1e30
F32 = jnp.float32
BF16 = jnp.bfloat16
MESH = pl.DeviceIdType.MESH
N_CLEAR = 4
VMEM_LIMIT = 65798144


def decode_kernel(
    n_sp, n_tp,
    len_hbm, xin_hbm, wq_hbm, wk_hbm, wv_hbm, wo_hbm, wg_hbm, wu_hbm, wd_hbm, ga_hbm, gm_hbm, kc_hbm, vc_hbm,
    xo_ref, kn_ref, vn_ref,
    wqkv, wo, wg, wu, wd, kbuf, vbuf, xin, qkvf, qacc, snew, obuf, stsend, orecv, strecv, o2d,
    gacc, uacc, act, psend, prev, precv, xres, xbuf, len_ref, ga_ref, gm_ref, sqsend, sqrecv,
    sem_x, sem_in, sem_qkv, sem_wo, sem_wg, sem_wu, sem_wd, sem_kv,
    ys_send, ys_recv, yt_send, yt_recv, yq_send, yq_recv,
    rs_send, rs_recv, ag_send, ag_recv, sq_send, sq_recv,
    f1_send, f1_recv, f2_send, f2_recv, f3_send, f3_recv,
):
    scope = jax.named_scope
    n_layers = wq_hbm.shape[0]
    batch, width = xin.shape
    head = kbuf.shape[1]
    qw = wq_hbm.shape[2]
    group = qw // head
    t_local = kbuf.shape[0] // batch
    rows = batch // n_sp
    cols = width // n_tp
    n_k = sem_qkv.shape[0]
    k_chunk = width // n_k
    n_gk = wg.shape[0]
    g_chunk = wg.shape[1]
    scale = head ** -0.5
    blk = rows * group
    sub = 16
    span = 4 * t_local
    s_idx = lax.axis_index("sp")
    i_idx = lax.axis_index("tp")

    def tp_peer(d):
        it, u = d // 2, d % 2
        near = (it * (3 - it)) // 2
        chips = near * (1 + 2 * u) + (1 - near) * (2 - 2 * (it // 3))
        flip = near * (2 - it) + (1 - near) * (1 - u)
        core = i_idx % 2
        return 2 * ((i_idx // 2 + chips) % (n_tp // 2)) + core + flip * (1 - 2 * core)

    def qkv_copies(l, c):
        ks = pl.ds(c * k_chunk, k_chunk)
        return (
            pltpu.make_async_copy(wq_hbm.at[l, ks, :], wqkv.at[ks, pl.ds(0, qw)], sem_qkv.at[c, 0]),
            pltpu.make_async_copy(wk_hbm.at[l, ks, :], wqkv.at[ks, pl.ds(qw, head)], sem_qkv.at[c, 1]),
            pltpu.make_async_copy(wv_hbm.at[l, ks, :], wqkv.at[ks, pl.ds(qw + head, head)], sem_qkv.at[c, 2]),
        )

    def wo_copy(l):
        return pltpu.make_async_copy(wo_hbm.at[l], wo, sem_wo)

    def wg_copy(l, c):
        return pltpu.make_async_copy(wg_hbm.at[l, pl.ds(pl.multiple_of(c * g_chunk, g_chunk), g_chunk), :], wg.at[c], sem_wg.at[c])

    def wu_copy(l, c):
        return pltpu.make_async_copy(wu_hbm.at[l, pl.ds(pl.multiple_of(c * g_chunk, g_chunk), g_chunk), :], wu.at[c], sem_wu.at[c])

    def wd_copy(l):
        return pltpu.make_async_copy(wd_hbm.at[l], wd, sem_wd)

    def kv_copies(l):
        return (
            pltpu.make_async_copy(kc_hbm.at[l], kbuf, sem_kv.at[0]),
            pltpu.make_async_copy(vc_hbm.at[l], vbuf, sem_kv.at[1]),
        )

    n_x_pieces = sem_x.shape[0]
    x_piece = batch // n_x_pieces
    x_copies = [
        pltpu.make_async_copy(
            xin_hbm.at[pl.ds(p * x_piece, x_piece), :], xin.at[pl.ds(p * x_piece, x_piece), :], sem_x.at[p])
        for p in range(n_x_pieces)
    ]
    for cp in x_copies:
        cp.start()
    ga_copy = pltpu.make_async_copy(ga_hbm, ga_ref, sem_in.at[0])
    gm_copy = pltpu.make_async_copy(gm_hbm, gm_ref, sem_in.at[1])
    len_copy = pltpu.make_async_copy(len_hbm, len_ref, sem_in.at[2])
    ga_copy.start()

    @pl.loop(0, N_CLEAR)
    def _(r):
        gacc[...] = jnp.zeros(gacc.shape, F32)
        uacc[...] = jnp.zeros(uacc.shape, F32)

    for c in range(n_k // 2):
        for cp in qkv_copies(0, c):
            cp.start()
    gm_copy.start()
    len_copy.start()

    barrier = pltpu.get_barrier_semaphore()
    for e in range(1, n_sp):
        pl.semaphore_signal(barrier, inc=1, device_id={"sp": lax.rem(s_idx + e, n_sp)}, device_id_type=MESH)
    for d in range(1, n_tp):
        pl.semaphore_signal(barrier, inc=1, device_id={"tp": lax.rem(i_idx + d, n_tp)}, device_id_type=MESH)

    def norm_block(load, store, gain_ref, l):
        total = None
        for c in range(n_tp):
            v = load(c).astype(F32)
            total = v * v if total is None else total + v * v
        mean_sq = jnp.sum(total, axis=-1, keepdims=True) * (1.0 / width)
        inv = lax.rsqrt(mean_sq + EPSILON)
        for c in range(n_tp):
            gain = gain_ref[pl.ds(l, 1), pl.ds(c * cols, cols)].astype(F32)
            store(c, (load(c).astype(F32) * inv * gain).astype(BF16))

    my_rows = pl.ds(pl.multiple_of(s_idx * rows, rows), rows)
    my_cols = pl.ds(pl.multiple_of(i_idx * cols, cols), cols)

    with scope("x_wait"):
        for cp in x_copies:
            cp.wait()
    for c in range(n_k // 2, n_k):
        for cp in qkv_copies(0, c):
            cp.start()
    xres[...] = xin[my_rows, my_cols]

    ga_copy.wait()
    with scope("norm"):
        @pl.loop(0, n_sp)
        def _(r):
            rs = pl.ds(pl.multiple_of(r * rows, rows), rows)

            def store(c, v):
                xin[rs, pl.ds(c * cols, cols)] = v

            norm_block(lambda c: xin[rs, pl.ds(c * cols, cols)], store, ga_ref, 0)

    kv_copies(0)[0].start()

    def sp_copies(e):
        t = lax.rem(s_idx + e, n_sp)
        return (
            pltpu.make_async_remote_copy(
                src_ref=stsend.at[t], dst_ref=strecv.at[e - 1], send_sem=yt_send.at[e - 1],
                recv_sem=yt_recv.at[e - 1], device_id={"sp": t}, device_id_type=MESH),
            pltpu.make_async_remote_copy(
                src_ref=obuf.at[t], dst_ref=orecv.at[e - 1], send_sem=ys_send.at[e - 1],
                recv_sem=ys_recv.at[e - 1], device_id={"sp": t}, device_id_type=MESH),
        )

    def qkv_copy(l, e, part):
        at = (l, my_rows, pl.ds(part * qw, qw + part * (2 * head - qw)))
        return pltpu.make_async_remote_copy(
            src_ref=qkvf.at[at], dst_ref=qkvf.at[at], send_sem=yq_send.at[part, e - 1],
            recv_sem=yq_recv.at[part, e - 1], device_id={"sp": lax.rem(s_idx + e, n_sp)}, device_id_type=MESH)

    n_sub = rows // sub
    tall = group * sub
    which = lax.rem(lax.broadcasted_iota(jnp.int32, (tall, span), 0), sub) // 4
    eye = lax.broadcasted_iota(jnp.int32, (blk, blk), 0) == lax.broadcasted_iota(jnp.int32, (blk, blk), 1)

    def score_rows(l, t):
        scores = []
        for u in range(n_sub):
            r0 = pl.multiple_of(t * rows + u * sub, sub)
            q64 = jnp.concatenate([qkvf[l, pl.ds(r0, sub), pl.ds(g * head, head)] for g in range(group)], axis=0)
            k16 = kbuf[pl.ds(pl.multiple_of(r0 * t_local, sub * t_local), sub * t_local), :]
            s4 = lax.dot_general(q64, k16, (((1,), (1,)), ((), ())), preferred_element_type=F32)
            comb = s4[:, 0:span]
            for j in range(1, sub // 4):
                comb = jnp.where(which == j, s4[:, j * span:(j + 1) * span], comb)
            scores.append(comb * scale)
        return jnp.concatenate(scores, axis=0)

    def attend(t, score):
        row_b = lax.broadcasted_iota(jnp.int32, (blk, batch), 0)
        row_b = t * rows + (row_b // tall) * sub + lax.rem(row_b, sub)
        lane_b = lax.broadcasted_iota(jnp.int32, (blk, batch), 1)
        lens = len_ref[...].astype(F32)
        len_row = jnp.sum(jnp.where(row_b == lane_b, lens, 0.0), axis=1, keepdims=True)
        lane = lax.broadcasted_iota(jnp.int32, (blk, span), 1)
        row = lax.broadcasted_iota(jnp.int32, (blk, span), 0)
        pos = (lax.rem(lane, t_local) + s_idx * t_local).astype(F32)
        valid = jnp.logical_and(lane // t_local == lax.rem(row, 4), pos < len_row)
        score = jnp.where(valid, score, NEG_BIG)
        top = jnp.max(score, axis=-1, keepdims=True)
        prob = jnp.where(valid, jnp.exp(score - top), 0.0)
        tot = jnp.sum(prob, axis=-1, keepdims=True)
        stsend[t, pl.ds(0, 1), :] = jnp.sum(jnp.where(eye, top, 0.0), axis=0, keepdims=True)
        stsend[t, pl.ds(1, 1), :] = jnp.sum(jnp.where(eye, tot, 0.0), axis=0, keepdims=True)
        for u in range(n_sub):
            pr = prob[u * tall:(u + 1) * tall]
            wide = jnp.concatenate([jnp.where(which == j, pr, 0.0).astype(BF16) for j in range(sub // 4)], axis=1)
            v0 = pl.multiple_of((t * rows + u * sub) * t_local, sub * t_local)
            obuf[t, pl.ds(u * tall, tall), :] = jnp.dot(
                wide, vbuf[pl.ds(v0, sub * t_local), :], preferred_element_type=F32).astype(BF16)

    def attention(l):
        kv_copies(l)[0].wait()
        if l == 0:
            gm_copy.wait()
            len_copy.wait()
        order = (2, 1, 3, 0) if l == 0 else (0, 2, 1, 3)
        ahead = None
        for n, e in enumerate(order):
            t = lax.rem(s_idx + e, n_sp)
            score = score_rows(l, t) if ahead is None else ahead
            ahead = None
            if n + 1 < n_sp and (l == 0 or e > 0):
                if l > 0:
                    qkv_copy(l, n_sp - order[n + 1], 0).wait()
                ahead = score_rows(l, lax.rem(s_idx + order[n + 1], n_sp))
            if n == 0:
                kv_copies(l)[1].wait()
            attend(t, score)
            if l > 0 and e == 0:
                qkv_copy(l, n_sp - order[n + 1], 0).wait()
            if l == 0 and n == 1:
                for c in range(n_gk):
                    wg_copy(0, c).start()
                    wu_copy(0, c).start()
            if l == 0 and n == 0:
                pl.semaphore_wait(barrier, n_sp + n_tp - 2)
            if e > 0:
                for cp in sp_copies(e):
                    cp.start()
        my_q = [qkvf[l, my_rows, pl.ds(g * head, head)].astype(F32) for g in range(group)]
        my_k = qkvf[l, my_rows, pl.ds(qw, head)].astype(F32)
        news = [jnp.sum(q * my_k, axis=-1, keepdims=True) * scale for q in my_q]
        for u in range(n_sub):
            for g in range(group):
                snew[pl.ds((u * group + g) * sub, sub), :] = news[g][u * sub:(u + 1) * sub]
        if l + 1 < n_layers:
            for cp in kv_copies(l + 1):
                cp.start()

    def combine_over_sp(l):
        def column(v):
            return jnp.sum(jnp.where(eye, v, 0.0), axis=1, keepdims=True)

        sn = snew[...]
        tops = [column(stsend[s_idx, pl.ds(0, 1), :])]
        tots = [column(stsend[s_idx, pl.ds(1, 1), :])]
        parts = [obuf[s_idx]]
        with scope("sp_wait"):
            for e in range(1, n_sp):
                for cp in sp_copies(e):
                    cp.wait()
        for e in range(1, n_sp):
            tops.append(column(strecv[e - 1, pl.ds(0, 1), :]))
            tots.append(column(strecv[e - 1, pl.ds(1, 1), :]))
            parts.append(orecv[e - 1])
        run_max = sn
        for m in tops:
            run_max = jnp.maximum(run_max, m)
        p_new = jnp.exp(sn - run_max)
        denom = p_new
        v_own = qkvf[l, my_rows, pl.ds(qw + head, head)].astype(F32)
        v_rows = jnp.concatenate([v_own[b * sub:(b + 1) * sub] for b in range(n_sub) for _ in range(group)], axis=0)
        numer = p_new.astype(BF16).astype(F32) * v_rows
        for m, tt, o in zip(tops, tots, parts):
            w = jnp.exp(m - run_max)
            denom = denom + w * tt
            numer = numer + w * o.astype(F32)
        res = (numer / denom).astype(BF16)
        for b in range(n_sub):
            for g in range(group):
                a0 = (b * group + g) * sub
                o2d[pl.ds(b * sub, sub), pl.ds(g * head, head)] = res[a0:a0 + sub, :]

    def rs_copy(d, j):
        return pltpu.make_async_remote_copy(
            src_ref=psend.at[d], dst_ref=precv.at[d], send_sem=rs_send.at[d], recv_sem=rs_recv.at[d],
            device_id={"tp": j}, device_id_type=MESH)

    def reduce_over_tp(lhs_ref, w_ref, step):
        @pl.loop(0, n_tp // step)
        def _(it):
            for u in range(step):
                d = it * step + u
                part = jnp.dot(lhs_ref[...], w_ref[:, pl.ds(pl.multiple_of(tp_peer(d) * cols, cols), cols)],
                               preferred_element_type=F32)
                if u < step - 1:
                    psend[d] = part.astype(BF16)
                else:
                    @pl.when(d < n_tp - 1)
                    def _():
                        psend[d] = part.astype(BF16)

                    @pl.when(d == n_tp - 1)
                    def _():
                        prev[...] = part
            for u in range(step):
                d = it * step + u
                if u < step - 1:
                    rs_copy(d, tp_peer(d)).start()
                else:
                    @pl.when(d < n_tp - 1)
                    def _():
                        rs_copy(d, tp_peer(d)).start()

        with scope("reduce"):
            acc = prev[...]
            for d in range(n_tp - 1):
                rs_copy(d, tp_peer(d)).wait()
                acc = acc + precv[d].astype(F32)
        xres[...] = (xres[...].astype(F32) + acc).astype(BF16)

    def ag_copy(d):
        return pltpu.make_async_remote_copy(
            src_ref=xres, dst_ref=xbuf.at[i_idx], send_sem=ag_send.at[d], recv_sem=ag_recv.at[d],
            device_id={"tp": tp_peer(d)}, device_id_type=MESH)

    def sq_copy(d):
        return pltpu.make_async_remote_copy(
            src_ref=sqsend, dst_ref=sqrecv.at[i_idx], send_sem=sq_send.at[d], recv_sem=sq_recv.at[d],
            device_id={"tp": tp_peer(d)}, device_id_type=MESH)

    eye_sq = lax.broadcasted_iota(jnp.int32, (rows, 128), 0) == lax.broadcasted_iota(jnp.int32, (rows, 128), 1)

    def gather_start():
        own = xres[...].astype(F32)
        own_sq = jnp.sum(own * own, axis=-1, keepdims=True)
        sqsend[pl.ds(0, 1), :] = jnp.sum(jnp.where(eye_sq, own_sq, 0.0), axis=0, keepdims=True)
        for d in range(n_tp - 1):
            sq_copy(d).start()
        for d in range(n_tp - 1):
            ag_copy(d).start()
        xbuf[i_idx] = xres[...]
        sqrecv[i_idx] = sqsend[...]

    def gather_factor():
        for d in range(n_tp - 1):
            sq_copy(d).wait()
        total = sqrecv[0, pl.ds(0, 1), :]
        for j in range(1, n_tp):
            total = total + sqrecv[j, pl.ds(0, 1), :]
        mean_sq = jnp.sum(jnp.where(eye_sq, total, 0.0), axis=1, keepdims=True) * (1.0 / width)
        return lax.rsqrt(mean_sq + EPSILON)

    landing = ((0, (6,)), (1, (3, 5)), (3, (2, 4)), (2, (0, 1)))

    def gathered(gain_ref, l, inv, chips, slots):
        for d in slots:
            ag_copy(d).wait()
        chip = lax.rem(i_idx // 2 + chips, n_tp // 2)
        parts = []
        for u in range(2):
            j = 2 * chip + u
            gain = gain_ref[pl.ds(l, 1), pl.ds(pl.multiple_of(j * cols, cols), cols)].astype(F32)
            parts.append((xbuf[j].astype(F32) * inv * gain).astype(BF16))
        return chip, jnp.concatenate(parts, axis=1)

    for l in range(n_layers):
        if l == 0:
            with scope("qkv"):
                for c0 in (0, n_k // 2):
                    for c in range(c0, c0 + n_k // 2):
                        for cp in qkv_copies(l, c):
                            cp.wait()
                    ks = pl.ds(c0 * k_chunk, n_k // 2 * k_chunk)
                    part = jnp.dot(xin[:, ks], wqkv[ks, :], preferred_element_type=F32)
                    if c0 == 0:
                        qacc[...] = part
                        kv_copies(l)[1].start()
                        wo_copy(l).start()
                    else:
                        qkvf[l] = (qacc[...] + part).astype(BF16)
        else:
            with scope("gather_a"):
                gather_start()
                for c in range(n_k):
                    for cp in qkv_copies(l, c):
                        cp.wait()
                inv = gather_factor()
            with scope("qkv"):
                acc = None
                for chips, slots in landing:
                    chip, hk = gathered(ga_ref, l, inv, chips, slots)
                    ks = pl.ds(pl.multiple_of(chip * 2 * cols, 2 * cols), 2 * cols)
                    part = jnp.dot(hk, wqkv[ks, :], preferred_element_type=F32)
                    acc = part if acc is None else acc + part
                qkvf[l, my_rows, :] = acc.astype(BF16)
                if l + 1 < n_layers:
                    for c in range(n_k):
                        for cp in qkv_copies(l + 1, c):
                            cp.start()
            for part in range(2):
                for e in (2, 1, 3):
                    qkv_copy(l, e, part).start()
        with scope("attention"):
            attention(l)
        if l == 0:
            wd_copy(0).start()
        with scope("combine"):
            combine_over_sp(l)
        with scope("wo"):
            wo_copy(l).wait()
            reduce_over_tp(o2d, wo, 2)
        if l + 1 < n_layers:
            wo_copy(l + 1).start()
        with scope("gather_m"):
            gather_start()
            if l == 0 and n_layers > 1:
                for c in range(n_k):
                    for cp in qkv_copies(1, c):
                        cp.start()
            if l > 0:
                for e in range(1, n_sp):
                    qkv_copy(l, e, 1).wait()
            kn_ref[l] = qkvf[l, :, pl.ds(qw, head)]
            vn_ref[l] = qkvf[l, :, pl.ds(qw + head, head)]
            gacc[...] = jnp.zeros(gacc.shape, F32)
            uacc[...] = jnp.zeros(uacc.shape, F32)
            inv = gather_factor()
        with scope("gate_up"):
            for chips, slots in landing:
                chip, hk = gathered(gm_ref, l, inv, chips, slots)
                wg_copy(l, chip).wait()
                wu_copy(l, chip).wait()
                gacc[...] += jnp.dot(hk, wg[chip], preferred_element_type=F32)
                uacc[...] += jnp.dot(hk, wu[chip], preferred_element_type=F32)
                if l + 1 < n_layers:
                    wg_copy(l + 1, chip).start()
                    wu_copy(l + 1, chip).start()

            act[...] = (jax.nn.silu(gacc[...]) * uacc[...]).astype(BF16)
        with scope("down"):
            wd_copy(l).wait()
            reduce_over_tp(act, wd, 2)
        if l + 1 < n_layers:
            wd_copy(l + 1).start()

    n_x = n_tp // 2
    half = rows // 2
    partner = i_idx + 1 - 2 * lax.rem(i_idx, 2)

    def block(e, d, r0, n):
        t = lax.rem(s_idx + n_sp - e, n_sp)
        j = lax.rem(i_idx + n_tp - 2 * d, n_tp)
        return xo_ref.at[pl.ds(pl.multiple_of(t * rows + r0, half), n), pl.ds(pl.multiple_of(j * cols, cols), cols)]

    def send_sp(ref, e, k):
        return pltpu.make_async_remote_copy(
            src_ref=ref, dst_ref=ref, send_sem=f1_send.at[k], recv_sem=f1_recv.at[k],
            device_id={"sp": lax.rem(s_idx + e, n_sp)}, device_id_type=MESH)

    def send_x(ref, d, k):
        return pltpu.make_async_remote_copy(
            src_ref=ref, dst_ref=ref, send_sem=f2_send.at[k], recv_sem=f2_recv.at[k],
            device_id={"tp": lax.rem(i_idx + 2 * d, n_tp)}, device_id_type=MESH)

    def send_core(ref, k):
        return pltpu.make_async_remote_copy(
            src_ref=ref, dst_ref=ref, send_sem=f3_send.at[k], recv_sem=f3_recv.at[k],
            device_id={"tp": partner}, device_id_type=MESH)

    sent = []

    def go(cp):
        cp.start()
        sent.append(cp)

    with scope("final"):
        xo_ref[my_rows, my_cols] = xres[...]
        far_sp = sorted(range(1, n_sp), key=lambda e: -min(e, n_sp - e))
        far_x = sorted(range(1, n_x), key=lambda d: -min(d, n_x - d))
        own_upper, own_lower = block(0, 0, 0, half), block(0, 0, half, half)
        for first, second, late in ((own_upper, own_lower, 0), (own_lower, own_upper, 1)):
            for e, d in itertools.zip_longest(far_sp, far_x):
                if e is not None:
                    go(send_sp(first, e, late * (n_sp - 1) * n_x + e - 1))
                if d is not None:
                    go(send_x(second, d, late * (n_x - 1) * n_sp + d - 1))
        core = []

        def to_core(ref):
            cp = send_core(ref, len(core))
            core.append(cp)
            go(cp)

        to_core(block(0, 0, 0, rows))
        for e, d in itertools.zip_longest(far_sp[::-1], far_x[::-1]):
            if e is not None:
                ref = block(e, 0, 0, half)
                send_sp(ref, e, e - 1).wait_recv()
                for d2 in far_x:
                    go(send_x(ref, d2, (n_x - 1) * e + d2 - 1))
                to_core(ref)
            if d is not None:
                ref = block(0, d, half, half)
                send_x(ref, d, d - 1).wait_recv()
                for e2 in far_sp:
                    go(send_sp(ref, e2, (n_sp - 1) * d + e2 - 1))
                to_core(ref)
        for e, d in itertools.zip_longest(far_sp[::-1], far_x[::-1]):
            if e is not None:
                ref = block(e, 0, half, half)
                send_sp(ref, e, (n_sp - 1) * n_x + e - 1).wait_recv()
                to_core(ref)
            if d is not None:
                ref = block(0, d, 0, half)
                send_x(ref, d, (n_x - 1) * n_sp + d - 1).wait_recv()
                to_core(ref)
        for e in far_sp[::-1]:
            for d in far_x[::-1]:
                ref = block(e, d, 0, half)
                send_x(ref, d, (n_x - 1) * e + d - 1).wait_recv()
                to_core(ref)
                ref = block(e, d, half, half)
                send_sp(ref, e, (n_sp - 1) * d + e - 1).wait_recv()
                to_core(ref)
        for cp in core:
            cp.wait_recv()
        for cp in sent:
            cp.wait_send()


def write_out(x_ref, k_ref, v_ref, x_hbm, k_hbm, v_hbm, sem):
    copies = [
        pltpu.make_async_copy(x_ref, x_hbm, sem.at[0]),
        pltpu.make_async_copy(k_ref, k_hbm, sem.at[1]),
        pltpu.make_async_copy(v_ref, v_hbm, sem.at[2]),
    ]
    for cp in copies:
        cp.start()
    for cp in copies:
        cp.wait()


def solution(mesh):
    weight_col = P(None, None, "tp")
    weight_row = P(None, "tp", None)
    cache_spec = P(None, "dp", "tp", "sp", None)
    new_spec = P(None, "dp", "tp", None)
    n_sp = mesh.shape["sp"]
    n_tp = mesh.shape["tp"]

    def device_step(x_in, lengths, w_q, w_k, w_v, w_o, w_gate, w_up, w_down, gain_attn, gain_mlp, k_cache, v_cache):
        n_layers, width, qw = w_q.shape
        batch = x_in.shape[0]
        t_local, head = k_cache.shape[3], k_cache.shape[4]
        ff = w_gate.shape[2]
        group = qw // head
        rows, cols = batch // n_sp, width // n_tp
        n_k, n_gk = 4, n_tp // 2
        kc = k_cache.reshape(n_layers, batch * t_local, head)
        vc = v_cache.reshape(n_layers, batch * t_local, head)
        vm = pl.BlockSpec(memory_space=pltpu.VMEM)
        hbm = pl.BlockSpec(memory_space=pl.ANY)
        dma = pltpu.SemaphoreType.DMA
        scratch = [
            pltpu.VMEM((width, qw + 2 * head), BF16),
            pltpu.VMEM((qw, width), BF16),
            pltpu.VMEM((n_gk, width // n_gk, ff), BF16),
            pltpu.VMEM((n_gk, width // n_gk, ff), BF16),
            pltpu.VMEM((ff, width), BF16),
            pltpu.VMEM((batch * t_local, head), BF16),
            pltpu.VMEM((batch * t_local, head), BF16),
            pltpu.VMEM((batch, width), BF16),
            pltpu.VMEM((n_layers, batch, qw + 2 * head), BF16),
            pltpu.VMEM((batch, qw + 2 * head), F32),
            pltpu.VMEM((rows * group, 1), F32),
            pltpu.VMEM((n_sp, rows * group, head), BF16),
            pltpu.VMEM((n_sp, 8, rows * group), F32),
            pltpu.VMEM((n_sp - 1, rows * group, head), BF16),
            pltpu.VMEM((n_sp - 1, 8, rows * group), F32),
            pltpu.VMEM((rows, qw), BF16),
            pltpu.VMEM((rows, ff), F32),
            pltpu.VMEM((rows, ff), F32),
            pltpu.VMEM((rows, ff), BF16),
            pltpu.VMEM((n_tp - 1, rows, cols), BF16),
            pltpu.VMEM((rows, cols), F32),
            pltpu.VMEM((n_tp - 1, rows, cols), BF16),
            pltpu.VMEM((rows, cols), BF16),
            pltpu.VMEM((n_tp, rows, cols), BF16),
            pltpu.VMEM((1, batch), jnp.int32),
            pltpu.VMEM((n_layers, width), BF16),
            pltpu.VMEM((n_layers, width), BF16),
            pltpu.VMEM((8, 128), F32),
            pltpu.VMEM((n_tp, 8, 128), F32),
            dma((8,)), dma((3,)), dma((n_k, 3)), dma, dma((n_gk,)), dma((n_gk,)), dma, dma((2,)),
        ]
        scratch += [dma((n_sp - 1,))] * 4 + [dma((2, n_sp - 1))] * 2 + [dma((n_tp - 1,))] * 6
        n_x = n_tp // 2
        scratch += [dma(((n_sp - 1) * (n_x + 1),))] * 2 + [dma(((n_x - 1) * (n_sp + 1),))] * 2 + [dma((2 * n_sp * n_x - 1,))] * 2
        out_shape = (
            jax.ShapeDtypeStruct((batch, width), BF16),
            jax.ShapeDtypeStruct((n_layers, batch, head), BF16),
            jax.ShapeDtypeStruct((n_layers, batch, head), BF16),
        )
        results = pl.pallas_call(
            functools.partial(decode_kernel, n_sp, n_tp),
            out_shape=tuple(pltpu.VMEM(o.shape, o.dtype) for o in out_shape),
            in_specs=[hbm] * 13,
            out_specs=(vm, vm, vm),
            scratch_shapes=scratch,
            compiler_params=pltpu.CompilerParams(collective_id=0, has_side_effects=True, vmem_limit_bytes=VMEM_LIMIT),
            name="decode_layers",
        )(lengths.reshape(1, batch), x_in, w_q, w_k, w_v, w_o, w_gate, w_up, w_down, gain_attn, gain_mlp, kc, vc)
        x_out, k_new, v_new = pl.pallas_call(
            write_out,
            out_shape=out_shape,
            in_specs=[vm] * 3,
            out_specs=(hbm, hbm, hbm),
            scratch_shapes=[dma((3,))],
            name="write_out",
        )(*[pltpu.with_memory_space_constraint(r, pltpu.VMEM) for r in results])
        return x_out, k_new.reshape(n_layers, batch, 1, head), v_new.reshape(n_layers, batch, 1, head)

    in_specs = (P("dp", None), P("dp"), weight_col, weight_col, weight_col, weight_row, weight_col, weight_col, weight_row, P(None, None), P(None, None), cache_spec, cache_spec)
    out_specs = (P("dp", None), new_spec, new_spec)
    return jax.shard_map(device_step, mesh=mesh, in_specs=in_specs, out_specs=out_specs, check_vma=False)
```
